128 devices in a mesh: keys: 32 (over x, z, core), heads: 4 (over y).
Axes of the slice: x: 4, y: 4, z: 4, core: 2. Of those that a mesh axis runs over, the one named last changes fastest.
Arguments:
- queries: bfloat16 [64, 64, 128], P(None, 'heads'), may hold values from -128 to 128
- keys: bfloat16 [524288, 8, 128], P('keys', 'heads'), may hold values from -4 to 4
- values: bfloat16 [524288, 8, 128], P('keys', 'heads'), may hold values from -6 to 6
- out_weight: bfloat16 [8192, 8192], P('heads', 'keys'), may hold values from -0.0625 to 0.0625
- probe: bfloat16 [8192], P('keys'), may hold values from -6 to 6
- knocked: int32 [64, 16], replicated, may hold values from 0 to 127
Outputs:
- readout: float32 [64, 128], P(None, 'keys')
- picked: float32 [64, 16], replicated
The draws below stay inside these ranges and needn't reach their ends.
All inputs are finite; a program needn't handle non-finite values.
Results may differ from the reference program's by a relative error of at most 0.0003.
Values sent between devices are 32-bit elements; how exact they have to be, the bound alone decides.
No kernel may reach another device: no remote copies, remote signals or barrier semaphores. Data moves between devices by JAX's collectives and lax.ppermute only.
A program may use at most 128 MiB of HBM per device.

```python
import jax
import jax.numpy as jnp
from jax import lax

D = 8192
HEADS = 64
KV_HEADS = 8
HD = 128
NQ = 64
BLOCK = 4096
PICK = 16
BLOCKS = 128
CONTEXT = 524288


def masked_plan(key):
    count = max(1, min(3, NQ - 1))
    base = jax.random.fold_in(key, 31)
    askers = jax.random.permutation(jax.random.fold_in(base, 1), NQ - 1)[:count].astype(jnp.int32)
    offsets = jax.random.randint(jax.random.fold_in(base, 2), (count,), 0, NQ - 1 - askers)
    rows = CONTEXT - NQ + askers + 1 + offsets
    groups = jax.random.randint(jax.random.fold_in(base, 3), (count,), 0, KV_HEADS)
    within = jax.random.randint(jax.random.fold_in(base, 4), (count,), 0, HEADS // KV_HEADS)
    vectors = jnp.clip(jax.random.normal(jax.random.fold_in(base, 5), (count, HD), jnp.float32), -3.9, 3.9)
    return (rows, groups, within, askers, vectors)


def draw_keys(key, part):
    field = jnp.clip(jax.random.normal(jax.random.fold_in(key, 11), (CONTEXT, KV_HEADS, HD), jnp.float32), -4.0, 4.0)
    late_rows, late_groups, late_within, late_askers, late_vectors = masked_plan(key)
    field = field.at[late_rows, late_groups].set(late_vectors)
    return field.astype(jnp.bfloat16)


def draw_queries(key, part):
    field = 2.5 * jnp.clip(jax.random.normal(jax.random.fold_in(key, 21), (NQ, HEADS, HD), jnp.float32), -6.0, 6.0)
    late_rows, late_groups, late_within, late_askers, late_vectors = masked_plan(key)
    late_count = late_vectors.shape[0]
    late_strength = jnp.linspace(30.0, 60.0, late_count)
    late_scale = late_strength * HD ** 0.5 / jnp.sum(late_vectors * late_vectors, axis=1)
    late_heads = late_groups * (HEADS // KV_HEADS) + late_within
    field = field.at[late_askers, late_heads].set(late_scale[:, None] * late_vectors)
    field = jnp.clip(field, -128.0, 128.0)
    return field.astype(jnp.bfloat16)


def place_ends(values, own_key, low, largest):
    index_at = [jax.random.randint(jax.random.fold_in(own_key, axis), (), 0, length) for axis, length in enumerate(values.shape)]
    widest = values.shape.index(max(values.shape))
    next_to = index_at[:widest] + [(index_at[widest] + 1) % values.shape[widest]] + index_at[widest + 1:]
    return values.at[tuple(index_at)].set(low).at[tuple(next_to)].set(largest)


def block_levels(key, dims, cuts, low, largest):
    gain = 1.0
    for axis_at, blocks in cuts:
        draws = jax.random.uniform(jax.random.fold_in(jax.random.fold_in(key, 6), axis_at), (blocks,), jnp.float32, low / len(cuts), largest / len(cuts))
        gain = gain * jnp.repeat(jnp.exp(draws), dims[axis_at] // blocks).reshape((-1,) + (1,) * (len(dims) - 1 - axis_at))
    return gain


def gaussian(own_key, shape, scale, limit, cuts=(), held_as=jnp.bfloat16):
    gain = block_levels(own_key, shape, cuts, -0.22, 0.18) if cuts else 1.0
    drawn = jax.random.normal(own_key, shape, jnp.float32) * scale * gain
    return jnp.minimum(jnp.maximum(drawn, -limit), limit).astype(held_as)


def setup_inputs(seed: int = 0) -> dict:
    seeds = jax.random.split(jax.random.key(seed), 7)
    queries = draw_queries(jax.random.fold_in(seeds[6], 71), 0)
    keys = draw_keys(jax.random.fold_in(seeds[6], 71), 0)
    values = gaussian(seeds[2], (CONTEXT, KV_HEADS, HD), 1.0, 6.0, ((0, 32), (1, 4)))
    out_weight = gaussian(seeds[3], (HEADS * HD, D), (HEADS * HD) ** -0.5, 0.0625, ((0, 4), (1, 32)))
    probe = gaussian(seeds[4], (D,), 1.0, 6.0, ((0, 32),))
    knocked = place_ends(jax.random.randint(seeds[5], (NQ, PICK), 0, BLOCKS), jax.random.fold_in(seeds[5], 1), 0, BLOCKS - 1).astype(jnp.int32)
    return {"queries": queries, "keys": keys, "values": values, "out_weight": out_weight, "probe": probe, "knocked": knocked}


NEG = -1e30


def combine(first, second):
    m1, s1, o1 = first
    m2, s2, o2 = second
    top = jnp.maximum(m1, m2)
    a = jnp.exp(m1 - top)
    b = jnp.exp(m2 - top)
    return top, s1 * a + s2 * b, o1 * a[..., None] + o2 * b[..., None]


def reference(queries, keys, values, out_weight, probe, knocked):
    group = HEADS // KV_HEADS
    direction = jnp.dot(out_weight, probe, preferred_element_type=jnp.float32).reshape(KV_HEADS, group, HD)
    grouped = queries.astype(jnp.float32).reshape(NQ, KV_HEADS, group, HD)
    key_blocks = keys.reshape(BLOCKS, BLOCK, KV_HEADS, HD)
    value_blocks = values.reshape(BLOCKS, BLOCK, KV_HEADS, HD)
    query_pos = CONTEXT - NQ + jnp.arange(NQ, dtype=jnp.int32)

    def block_state(index):
        kblk = lax.dynamic_index_in_dim(key_blocks, index, 0, False).astype(jnp.float32)
        vblk = lax.dynamic_index_in_dim(value_blocks, index, 0, False).astype(jnp.float32)
        scores = jnp.einsum("qgrd,kgd->qgrk", grouped, kblk) * (HD ** -0.5)
        key_pos = index * BLOCK + jnp.arange(BLOCK, dtype=jnp.int32)
        allowed = key_pos[None, :] <= query_pos[:, None]
        scores = jnp.where(allowed[:, None, None, :], scores, NEG)
        top = jnp.max(scores, axis=-1)
        weights = jnp.exp(scores - top[..., None])
        total = jnp.sum(weights, axis=-1)
        summed = jnp.einsum("qgrk,kgd->qgrd", weights.astype(jnp.bfloat16).astype(jnp.float32), vblk)
        return top, total, summed

    states = lax.map(block_state, jnp.arange(BLOCKS, dtype=jnp.int32))
    empty = (jnp.full((NQ, KV_HEADS, group), NEG, jnp.float32),
             jnp.zeros((NQ, KV_HEADS, group), jnp.float32),
             jnp.zeros((NQ, KV_HEADS, group, HD), jnp.float32))

    def forward(carry, item):
        return combine(carry, item), carry

    _, before = lax.scan(forward, empty, states)
    _, after = lax.scan(forward, empty, states, reverse=True)
    top, total, summed = combine(before, after)
    projected = jnp.sum(summed * direction, axis=-1)
    readout = jnp.sum(projected / total, axis=(2, 3)).T
    picked = jnp.take_along_axis(readout, knocked, axis=1)
    return readout, picked
```

```python
import functools

import jax
import jax.numpy as jnp
from jax import lax
from jax.experimental import pallas as pl
from jax.experimental.pallas import tpu as pltpu
from jax.sharding import Mesh, PartitionSpec as P

BLOCK = 4096
KEY_AXES = (4, 4, 2)
NEG = -1e30
SCALE2 = 128 ** -0.5 * 1.4426950408889634
HIGH = lax.Precision.HIGHEST
F32 = jnp.float32


def attn_kernel(base_ref, q_ref, k_ref, v_ref, ms_ref, o_ref, qt, sc, *, T1, T2, nblk, context, nq):
    b = pl.program_id(0)
    rows = k_ref.shape[0]
    R = qt.shape[1]
    hd = k_ref.shape[1]
    @pl.when(b == 0)
    def _():
        q = q_ref[...].astype(jnp.float32)
        g = q.shape[1] // 2
        both = jnp.concatenate([q[:, :g].reshape(R, hd), q[:, g:].reshape(R, hd)], axis=1)
        qt[...] = both.T.astype(jnp.bfloat16)

    def masked(x):
        par = lax.broadcasted_iota(jnp.int32, x.shape, 0) & 1
        even = (par == 0).astype(x.dtype)
        return jnp.concatenate([x * even, x * (1 - even)], axis=1)

    def first(i, mx):
        at = pl.ds(pl.multiple_of(i * T1, T1), T1)
        s = jnp.dot(masked(k_ref[at, :]), qt[...], preferred_element_type=jnp.float32)
        sc[at, :] = s
        return jnp.maximum(mx, jnp.max(s.reshape(T1 // 8, 8, R), axis=0))

    mx = lax.fori_loop(0, rows // T1, first, jnp.full((8, R), NEG, jnp.float32))
    tail = pl.ds(rows - 2 * nq, 2 * nq)

    @pl.when(base_ref[0] + (b + 1) * (rows // 2) == context)
    def _():
        s = sc[tail, :]
        key = lax.shift_right_logical(lax.broadcasted_iota(jnp.int32, s.shape, 0), 1)
        query = lax.div(lax.broadcasted_iota(jnp.int32, s.shape, 1), jnp.int32(R // nq))
        sc[tail, :] = jnp.where(key <= query, s, NEG)
    last = base_ref[0] + (b + 1) * (rows // 2) == context
    def fix(_):
        def again(i, mx):
            at = pl.ds(pl.multiple_of(i * 128, 128), 128)
            return jnp.maximum(mx, jnp.max(sc[at, :].reshape(16, 8, R), axis=0))
        return lax.fori_loop(0, rows // 128, again, jnp.full((8, R), NEG, jnp.float32))
    mx = lax.cond(last, fix, lambda _: mx, 0)
    mx = jnp.maximum(mx, pltpu.roll(mx, 2, 0))
    mx = jnp.maximum(mx, pltpu.roll(mx, 4, 0))

    o_ref[...] = jnp.zeros_like(o_ref)
    def second(i, tot):
        at = pl.ds(pl.multiple_of(i * T2, T2), T2)
        s = sc[at, :].reshape(T2 // 8, 8, R)
        p = jnp.exp2((s - mx[None]) * SCALE2)
        tot = tot + jnp.sum(p, axis=0)
        pb = p.reshape(T2, R).astype(jnp.bfloat16)
        o_ref[...] += lax.dot_general(masked(v_ref[at, :]), pb, (((0,), (0,)), ((), ())), preferred_element_type=jnp.float32)
        return tot
    tot = lax.fori_loop(0, rows // T2, second, jnp.zeros((8, R), jnp.float32))
    tot = tot + pltpu.roll(tot, 2, 0)
    tot = tot + pltpu.roll(tot, 4, 0)
    ms_ref[0:2, :] = mx[0:2] * SCALE2
    ms_ref[2:4, :] = tot[0:2]

def attention(base, queries, keys, values, block, context, T1=512, T2=512, interpret=False):
    nq, hq, hd = queries.shape
    n, kvh, _ = keys.shape
    R = nq * hq // kvh
    nblk = n // block
    rows = kvh * block
    k2 = keys.reshape(n * kvh, hd)
    v2 = values.reshape(n * kvh, hd)
    return pl.pallas_call(
        functools.partial(attn_kernel, T1=T1, T2=T2, nblk=nblk, context=context, nq=nq),
        grid=(nblk,),
        in_specs=[
            pl.BlockSpec(memory_space=pltpu.SMEM),
            pl.BlockSpec((nq, hq, hd), lambda b: (0, 0, 0)),
            pl.BlockSpec((rows, hd), lambda b: (b, 0)),
            pl.BlockSpec((rows, hd), lambda b: (b, 0)),
        ],
        out_specs=[
            pl.BlockSpec((None, 4, R), lambda b: (b, 0, 0)),
            pl.BlockSpec((None, kvh * hd, R), lambda b: (b, 0, 0)),
        ],
        out_shape=[
            jax.ShapeDtypeStruct((nblk, 4, R), jnp.float32),
            jax.ShapeDtypeStruct((nblk, kvh * hd, R), jnp.float32),
        ],
        scratch_shapes=[
            pltpu.VMEM((kvh * hd, R), jnp.bfloat16),
            pltpu.VMEM((rows, R), jnp.float32),
        ],
        compiler_params=pltpu.CompilerParams(vmem_limit_bytes=60 * 2**20),
        cost_estimate=pl.CostEstimate(flops=4 * R * n * kvh * hd * 2, bytes_accessed=2 * n * kvh * hd * 2, transcendentals=R * n * kvh),
        name="attention",
    )(base, queries, k2, v2)


def iota(shape, dim):
    return lax.broadcasted_iota(jnp.int32, shape, dim)


def direction_kernel(w_ref, p_ref, out_ref):
    part = lax.dot_general(p_ref[...], w_ref[...], (((1,), (1,)), ((), ())), preferred_element_type=F32)
    heads, hd = out_ref.shape[1:]
    rows = [part[0:1, h * hd:(h + 1) * hd] for h in range(heads)]
    full = jnp.concatenate(rows, axis=0)
    for dest in range(out_ref.shape[0]):
        out_ref[dest] = full


def direction_parts(out_weight, probe, hd, dests):
    rows, cols = out_weight.shape
    probe8 = jnp.broadcast_to(probe[None], (8, cols))
    return pl.pallas_call(
        direction_kernel,
        out_shape=jax.ShapeDtypeStruct((dests, rows // hd, hd), F32),
        cost_estimate=pl.CostEstimate(flops=2 * rows * cols, bytes_accessed=rows * cols * 2, transcendentals=0),
        name="direction",
    )(out_weight, probe8)


def pack_kernel(dir_ref, ms_ref, o_ref, out_ref, x):
    nblk, rows, R = o_ref.shape
    heads, hd = dir_ref.shape[1:]
    group = heads // 2
    direction = jnp.sum(dir_ref[...], axis=0)
    spread = (iota((group, 128), 1) & (group - 1)) == iota((group, 128), 0)
    spread = spread.astype(F32)
    for g in range(2):
        wide = lax.dot_general(direction[g * group:(g + 1) * group], spread, (((0,), (0,)), ((), ())),
                               preferred_element_type=F32, precision=HIGH)
        for b in range(nblk):
            at = g * nblk + b
            x[at:at + 1, :] = ms_ref[b, g:g + 1, :]
            x[8 + at:9 + at, :] = ms_ref[b, 2 + g:3 + g, :]
            for c in range(0, R, 128):
                part = o_ref[b, g * hd:(g + 1) * hd, c:c + 128] * wide
                x[16 + at:17 + at, c:c + 128] = jnp.sum(part, axis=0, keepdims=True)
    dests = out_ref.shape[0]
    share = R // 128
    for dest in range(dests):
        c = dest // (dests // share) * 128
        out_ref[dest] = x[:, c:c + 128]


def pack(gathered, ms, o):
    dests = gathered.shape[0]
    return pl.pallas_call(
        pack_kernel,
        out_shape=jax.ShapeDtypeStruct((dests, 24, 128), F32),
        scratch_shapes=[pltpu.VMEM((24, ms.shape[2]), F32)],
        cost_estimate=pl.CostEstimate(flops=2 * o.size, bytes_accessed=o.size * 4, transcendentals=0),
        name="pack",
    )(gathered, ms, o)


def turned(x, k):
    row = iota(x.shape, x.ndim - 2) & 3
    return jnp.where(row >= k, pltpu.roll(x, k, x.ndim - 2), pltpu.roll(x, k + 4, x.ndim - 2))


def around(x, op):
    x = op(x, turned(x, 1))
    return op(x, turned(x, 2))


def out_of_sources(x):
    n = x.shape[0]
    before = [jnp.zeros_like(x[0])]
    after = [jnp.zeros_like(x[0])]
    for k in range(n - 1):
        before.append(before[-1] + x[k])
        after.insert(0, after[0] + x[n - 1 - k])
    return jnp.stack([p + q for p, q in zip(before, after)], axis=0)


def leave_kernel(got_ref, out_ref):
    m = got_ref[:, 0:8, :]
    s = got_ref[:, 8:16, :]
    o = got_ref[:, 16:24, :]
    n = m.shape[0]
    top = around(jnp.max(m, axis=0), jnp.maximum)
    is_top = m == top[None]
    count = around(jnp.sum(is_top.astype(F32), axis=0), jnp.add)
    second = around(jnp.max(jnp.where(is_top, NEG, m), axis=0), jnp.maximum)
    factor = jnp.exp2(m - top[None])
    low = jnp.where(is_top, 0.0, jnp.exp2(jnp.minimum(m - second[None], 0.0)))
    alone = is_top & (count == 1.0)[None]

    def left_out(x):
        a = x * factor
        inner = turned(a, 1) + turned(a, 2) + turned(a, 3)
        shared = inner + out_of_sources(a + inner)
        rest = around(jnp.sum(x * low, axis=0), jnp.add)
        return jnp.where(alone, rest[None], shared)

    ratio = left_out(o) / left_out(s)
    both = ratio + pltpu.roll(ratio, 4, 1)
    pairs = both.reshape(n // 2, 2, 8, 128)
    dense = jnp.where(iota((n // 2, 8, 128), 1) < 4, pairs[:, 0], pairs[:, 1]).reshape(n * 4, 128)
    queries = out_ref.shape[1]
    per = 128 // queries
    pick = lax.div(iota((queries, 128), 1), jnp.int32(per)) == iota((queries, 128), 0)
    part = lax.dot_general(pick.astype(F32), dense, (((1,), (1,)), ((), ())), preferred_element_type=F32, precision=HIGH)
    for dest in range(out_ref.shape[0]):
        out_ref[dest] = part


def leave(got, queries, dests):
    return pl.pallas_call(
        leave_kernel,
        out_shape=jax.ShapeDtypeStruct((dests, queries, got.shape[0] * 4), F32),
        cost_estimate=pl.CostEstimate(flops=8 * got.size, bytes_accessed=got.size * 4, transcendentals=got.size),
        name="leave",
    )(got)


def finish_kernel(device_ref, got_ref, knocked_ref, read_ref, pick_ref, table):
    nx, ny, q, nb = got_ref.shape
    for i in range(nx):
        total = got_ref[i, 0]
        for j in range(1, ny):
            total = total + got_ref[i, j]
        table[i * q:(i + 1) * q, :] = total
    full = table[...].T
    block = iota(full.shape, 0)
    for k in range(pick_ref.shape[0]):
        here = jnp.where(block == knocked_ref[k:k + 1, :], full, 0.0)
        pick_ref[k:k + 1, :] = jnp.sum(here, axis=0, keepdims=True)
    nblk = read_ref.shape[0]
    for t in range(nblk):
        here = jnp.where(block == device_ref[0] * nblk + t, full, 0.0)
        read_ref[t:t + 1, :] = jnp.sum(here, axis=0, keepdims=True)


def finish(device, got, knocked_t, nblk):
    nx, ny, q, nb = got.shape
    vmem = pl.BlockSpec(memory_space=pltpu.VMEM)
    return pl.pallas_call(
        finish_kernel,
        in_specs=[pl.BlockSpec(memory_space=pltpu.SMEM), vmem, vmem],
        out_specs=[vmem, vmem],
        out_shape=[jax.ShapeDtypeStruct((nblk, nx * q), F32), jax.ShapeDtypeStruct(knocked_t.shape, F32)],
        scratch_shapes=[pltpu.VMEM((nx * q, nb), F32)],
        name="finish",
    )(device, got, knocked_t)


def body(queries, keys, values, out_weight, probe, knocked):
    nq, hq, hd = queries.shape
    nblk = keys.shape[0] // BLOCK
    axes = ("x", "z", "core")
    lanes = lax.axis_size(axes)
    device = lax.axis_index(axes).reshape(1)
    context = keys.shape[0] * lanes
    parts = direction_parts(out_weight, probe, hd, lanes)
    gathered = lax.all_to_all(parts, axes, 0, 0, tiled=True)
    ms, o = attention(device * keys.shape[0], queries, keys, values, BLOCK, context, 4096, 4096)
    got = lax.all_to_all(pack(gathered, ms, o), axes, 0, 0, tiled=True)
    nx, ny = lax.axis_size("x"), lax.axis_size("heads")
    sent = leave(got, nq // nx, nx * ny)
    back = lax.all_to_all(sent, ("x", "heads"), 0, 0, tiled=True)
    read, picked = finish(device, back.reshape(nx, ny, *back.shape[1:]), knocked.T, nblk)
    return read.T, picked.T


def solution(mesh):
    inner = Mesh(mesh.devices.reshape(*KEY_AXES, mesh.devices.shape[1]), ("x", "z", "core", "heads"))
    keys = ("x", "z", "core")
    in_specs = (
        P(None, "heads", None),
        P(keys, "heads", None),
        P(keys, "heads", None),
        P("heads", keys),
        P(keys),
        P(),
    )
    out_specs = (P(None, keys), P())
    return jax.shard_map(body, mesh=inner, in_specs=in_specs, out_specs=out_specs, check_vma=False)
```

```python
import functools

import jax
import jax.numpy as jnp
from jax import lax
from jax.experimental import pallas as pl
from jax.experimental.pallas import tpu as pltpu
from jax.sharding import Mesh, PartitionSpec as P

BLOCK = 4096
KEY_AXES = (4, 4, 2)
NEG = -1e30
SCALE2 = 128 ** -0.5 * 1.4426950408889634
HIGH = lax.Precision.HIGHEST
F32 = jnp.float32


def iota(shape, dim):
    return lax.broadcasted_iota(jnp.int32, shape, dim)


def small(mib):
    return pltpu.CompilerParams(vmem_limit_bytes=mib * 2**20)


def attn_kernel(base_ref, q_hbm, k_hbm, v_hbm, ms_ref, o_ref, q_ref, q_sem, qt, sc, k_ref, v_ref, k_sem, v_sem, *, C, nblk, context, nq):
    total = k_ref.shape[0]
    rows = total // nblk
    R = qt.shape[1]
    hd = k_ref.shape[1]
    per = rows // C
    late = 2 * nq

    def copy(hbm, ref, sem, i):
        at = pl.ds(pl.multiple_of(i * C, C), C)
        return pltpu.make_async_copy(hbm.at[at, :], ref.at[at, :], sem.at[i])

    queries = pltpu.make_async_copy(q_hbm, q_ref, q_sem.at[0])
    queries.start()
    for b in range(nblk):
        for i in range(per):
            copy(k_hbm, k_ref, k_sem, b * per + i).start()
        for i in range(per):
            copy(v_hbm, v_ref, v_sem, b * per + i).start()

    even = (1 - (lax.broadcasted_iota(jnp.int32, (16, hd), 0) & 1)).astype(jnp.bfloat16)
    odd = 1 - even
    lane_even = (1 - (lax.broadcasted_iota(jnp.int32, (16, 128), 1) & 1)).astype(jnp.bfloat16)
    le = jnp.concatenate([lane_even] * (rows // 128), axis=1)[None]

    queries.wait()
    q = q_ref[...].astype(F32)
    g = q.shape[1] // 2
    both = jnp.concatenate([q[:, :g].reshape(R, hd), q[:, g:].reshape(R, hd)], axis=1)
    qt[...] = both.T.astype(jnp.bfloat16)

    def masked(x):
        x3 = x.reshape(x.shape[0] // 16, 16, hd)
        return jnp.concatenate([(x3 * even[None]).reshape(x.shape), (x3 * odd[None]).reshape(x.shape)], axis=1)

    def top_of(s):
        return jnp.max(s.reshape(s.shape[0] // 8, 8, R), axis=0)

    def block(b, carry):
        here = pl.ds(pl.multiple_of(b * rows, rows), rows)
        for c in range(per):
            copy(k_hbm, k_ref, k_sem, b * per + c).wait()
        s = jnp.dot(masked(k_ref[here, :]), qt[...], preferred_element_type=jnp.float32) * SCALE2
        sc[...] = s
        early = top_of(s[:rows - late])

        def seen(_):
            tail = sc[rows - late:, :]
            key = lax.shift_right_logical(iota(tail.shape, 0), 1)
            query = lax.div(iota(tail.shape, 1), jnp.int32(R // nq))
            tail = jnp.where(key <= query, tail, NEG)
            sc[rows - late:, :] = tail
            return top_of(tail)

        last = base_ref[0] + (b + 1) * (rows // 2) == context
        mx = jnp.maximum(early, lax.cond(last, seen, lambda _: top_of(sc[rows - late:, :]), 0))
        mx = jnp.maximum(mx, pltpu.roll(mx, 2, 0))
        mx = jnp.maximum(mx, pltpu.roll(mx, 4, 0))

        for c in range(per):
            copy(v_hbm, v_ref, v_sem, b * per + c).wait()
        p = jnp.exp2(sc[...].reshape(rows // 8, 8, R) - mx[None])
        tot = jnp.sum(p, axis=0)
        pb = p.reshape(rows, R).astype(jnp.bfloat16)
        vt3 = v_ref[here, :].T.reshape(hd // 16, 16, rows)
        vt = jnp.concatenate([(vt3 * le).reshape(hd, rows), (vt3 * (1 - le)).reshape(hd, rows)], axis=0)
        o_ref[b] = jnp.dot(vt, pb, preferred_element_type=jnp.float32)
        tot = tot + pltpu.roll(tot, 2, 0)
        tot = tot + pltpu.roll(tot, 4, 0)
        ms_ref[b, 0:2, :] = mx[0:2]
        ms_ref[b, 2:4, :] = tot[0:2]
        return carry

    lax.fori_loop(0, nblk, block, 0)


def attention(base, queries, keys, values, block, context, C=2048, vl=48):
    nq, hq, hd = queries.shape
    n, kvh, _ = keys.shape
    R = nq * hq // kvh
    nblk = n // block
    rows = kvh * block
    k2 = keys.reshape(n * kvh, hd)
    v2 = values.reshape(n * kvh, hd)
    vmem = pl.BlockSpec(memory_space=pltpu.VMEM)
    hbm = pl.BlockSpec(memory_space=pltpu.HBM)
    return pl.pallas_call(
        functools.partial(attn_kernel, C=C, nblk=nblk, context=context, nq=nq),
        in_specs=[pl.BlockSpec(memory_space=pltpu.SMEM), hbm, hbm, hbm],
        out_specs=[vmem, vmem],
        out_shape=[
            jax.ShapeDtypeStruct((nblk, 4, R), jnp.float32),
            jax.ShapeDtypeStruct((nblk, kvh * hd, R), jnp.float32),
        ],
        scratch_shapes=[
            pltpu.VMEM(queries.shape, jnp.bfloat16),
            pltpu.SemaphoreType.DMA((1,)),
            pltpu.VMEM((kvh * hd, R), jnp.bfloat16),
            pltpu.VMEM((rows, R), jnp.float32),
            pltpu.VMEM((n * kvh, hd), jnp.bfloat16),
            pltpu.VMEM((n * kvh, hd), jnp.bfloat16),
            pltpu.SemaphoreType.DMA((n * kvh // C,)),
            pltpu.SemaphoreType.DMA((n * kvh // C,)),
        ],
        compiler_params=small(vl),
        cost_estimate=pl.CostEstimate(flops=4 * R * n * kvh * hd * 2, bytes_accessed=2 * n * kvh * hd * 2, transcendentals=R * n * kvh),
        name="attention",
    )(base, queries, k2, v2)


def direction_kernel(w_hbm, p_ref, out_ref, w, w_sem):
    copies = []
    step = w.shape[0] // w_sem.shape[0]
    for i in range(w_sem.shape[0]):
        at = pl.ds(i * step, step)
        copies.append(pltpu.make_async_copy(w_hbm.at[at, :], w.at[at, :], w_sem.at[i]))
        copies[-1].start()
    hd = out_ref.shape[2]
    probe = jnp.broadcast_to(p_ref[...].astype(F32).reshape(1, w.shape[1]), (8, w.shape[1])).astype(jnp.bfloat16)
    rows = []
    for i, c in enumerate(copies):
        c.wait()
        part = lax.dot_general(probe, w[i * step:(i + 1) * step, :], (((1,), (1,)), ((), ())), preferred_element_type=F32)
        rows += [part[0:1, h * hd:(h + 1) * hd] for h in range(step // hd)]
    full = jnp.concatenate(rows, axis=0)
    for dest in range(out_ref.shape[0]):
        out_ref[dest] = full


def direction_parts(out_weight, probe, hd, dests):
    rows, cols = out_weight.shape
    vmem = pl.BlockSpec(memory_space=pltpu.VMEM)
    hbm = pl.BlockSpec(memory_space=pltpu.HBM)
    return pl.pallas_call(
        direction_kernel,
        in_specs=[hbm, vmem],
        out_specs=vmem,
        out_shape=jax.ShapeDtypeStruct((dests, rows // hd, hd), F32),
        scratch_shapes=[
            pltpu.VMEM(out_weight.shape, jnp.bfloat16),
            pltpu.SemaphoreType.DMA((4,)),
        ],
        cost_estimate=pl.CostEstimate(flops=2 * rows * cols, bytes_accessed=rows * cols * 2, transcendentals=0),
        compiler_params=small(63),
        name="direction",
    )(out_weight, probe)


def pack_kernel(dir_ref, ms_ref, o_ref, out_ref, x):
    nblk, rows, R = o_ref.shape
    heads, hd = dir_ref.shape[1:]
    group = heads // 2
    direction = jnp.sum(dir_ref[...], axis=0)
    spread = (iota((group, 128), 1) & (group - 1)) == iota((group, 128), 0)
    spread = spread.astype(F32)
    for g in range(2):
        wide = lax.dot_general(direction[g * group:(g + 1) * group], spread, (((0,), (0,)), ((), ())),
                               preferred_element_type=F32, precision=HIGH)
        for b in range(nblk):
            at = g * nblk + b
            x[at:at + 1, :] = ms_ref[b, g:g + 1, :]
            x[8 + at:9 + at, :] = ms_ref[b, 2 + g:3 + g, :]
            for c in range(0, R, 128):
                part = o_ref[b, g * hd:(g + 1) * hd, c:c + 128] * wide
                x[16 + at:17 + at, c:c + 128] = jnp.sum(part, axis=0, keepdims=True)
    total = x[8:16, :]
    level = x[0:8, :] + jnp.log2(total)
    mean = x[16:24, :] / total
    dests = out_ref.shape[0]
    wide = out_ref.shape[2]
    for dest in range(dests):
        c = dest % (R // wide) * wide
        out_ref[dest, 0:8, :] = level[:, c:c + wide]
        out_ref[dest, 8:16, :] = mean[:, c:c + wide]


def pack(gathered, ms, o, shares):
    dests = gathered.shape[0]
    R = ms.shape[2]
    return pl.pallas_call(
        pack_kernel,
        out_shape=jax.ShapeDtypeStruct((dests, 16, R // shares), F32),
        scratch_shapes=[pltpu.VMEM((24, R), F32)],
        cost_estimate=pl.CostEstimate(flops=2 * o.size, bytes_accessed=o.size * 4, transcendentals=0),
        compiler_params=small(8),
        name="pack",
    )(gathered, ms, o)


def turned(x, k):
    row = iota(x.shape, x.ndim - 2) & 3
    return jnp.where(row >= k, pltpu.roll(x, k, x.ndim - 2), pltpu.roll(x, k + 4, x.ndim - 2))


def around(x, op):
    x = op(x, turned(x, 1))
    return op(x, turned(x, 2))


def out_of_sources(x):
    n = x.shape[0]
    before = [jnp.zeros_like(x[0])]
    after = [jnp.zeros_like(x[0])]
    for k in range(n - 1):
        before.append(before[-1] + x[k])
        after.insert(0, after[0] + x[n - 1 - k])
    return jnp.stack([p + q for p, q in zip(before, after)], axis=0)


def leave_kernel(got_ref, out_ref):
    level = got_ref[:, 0:8, :]
    mean = got_ref[:, 8:16, :]
    n, _, lanes = level.shape
    top = around(jnp.max(level, axis=0), jnp.maximum)
    is_top = level == top[None]
    count = around(jnp.sum(is_top.astype(F32), axis=0), jnp.add)
    second = around(jnp.max(jnp.where(is_top, NEG, level), axis=0), jnp.maximum)
    factor = jnp.exp2(level - top[None])
    low = jnp.where(is_top, 0.0, jnp.exp2(jnp.minimum(level - second[None], 0.0)))
    alone = is_top & (count == 1.0)[None]

    def left_out(a, rest):
        inner = turned(a, 1) + turned(a, 2) + turned(a, 3)
        shared = inner + out_of_sources(a + inner)
        rest = around(jnp.sum(rest, axis=0), jnp.add)
        return jnp.where(alone, rest[None], shared)

    ratio = left_out(mean * factor, mean * low) / left_out(factor, low)
    both = ratio + pltpu.roll(ratio, 4, 1)
    pairs = both.reshape(n // 2, 2, 8, lanes)
    dense = jnp.where(iota((n // 2, 8, lanes), 1) < 4, pairs[:, 0], pairs[:, 1]).reshape(n * 4, lanes)
    queries = out_ref.shape[1]
    per = lanes // queries
    pick = lax.div(iota((queries, lanes), 1), jnp.int32(per)) == iota((queries, lanes), 0)
    part = lax.dot_general(pick.astype(F32), dense, (((1,), (1,)), ((), ())), preferred_element_type=F32, precision=HIGH)
    for dest in range(out_ref.shape[0]):
        out_ref[dest] = part


def leave(got, queries, dests):
    return pl.pallas_call(
        leave_kernel,
        out_shape=jax.ShapeDtypeStruct((dests, queries, got.shape[0] * 4), F32),
        cost_estimate=pl.CostEstimate(flops=8 * got.size, bytes_accessed=got.size * 4, transcendentals=got.size),
        compiler_params=small(8),
        name="leave",
    )(got)


def finish_kernel(device_ref, got_ref, knocked_ref, read_ref, pick_ref):
    nx, ny, q, nb = got_ref.shape
    parts = []
    for i in range(nx):
        total = got_ref[i, 0]
        for j in range(1, ny):
            total = total + got_ref[i, j]
        parts.append(total)
    full = jnp.concatenate(parts, axis=0).T
    block = iota(full.shape, 0)
    for k in range(pick_ref.shape[0]):
        here = jnp.where(block == knocked_ref[k:k + 1, :], full, 0.0)
        pick_ref[k:k + 1, :] = jnp.sum(here, axis=0, keepdims=True)
    nblk = read_ref.shape[0]
    for t in range(nblk):
        here = jnp.where(block == device_ref[0] * nblk + t, full, 0.0)
        read_ref[t:t + 1, :] = jnp.sum(here, axis=0, keepdims=True)


def finish(device, got, knocked_t, nblk):
    nx, ny, q, nb = got.shape
    vmem = pl.BlockSpec(memory_space=pltpu.VMEM)
    return pl.pallas_call(
        finish_kernel,
        in_specs=[pl.BlockSpec(memory_space=pltpu.SMEM), vmem, vmem],
        out_specs=[vmem, vmem],
        out_shape=[jax.ShapeDtypeStruct((nblk, nx * q), F32), jax.ShapeDtypeStruct(knocked_t.shape, F32)],
        compiler_params=small(2),
        name="finish",
    )(device, got, knocked_t)


def body(queries, keys, values, out_weight, probe, knocked):
    nq, hq, hd = queries.shape
    nblk = keys.shape[0] // BLOCK
    axes = ("x", "z", "core")
    lanes = lax.axis_size(axes)
    device = lax.axis_index(axes).reshape(1)
    context = keys.shape[0] * lanes
    parts = direction_parts(out_weight, probe, hd, lanes)
    gathered = lax.all_to_all(parts, axes, 0, 0, tiled=True)
    ms, o = attention(device * keys.shape[0], queries, keys, values, BLOCK, context)
    shares, ny = lax.axis_size("core"), lax.axis_size("heads")
    got = lax.all_to_all(pack(gathered, ms, o, shares), axes, 0, 0, tiled=True)
    sent = leave(got, nq // shares, shares * ny)
    back = lax.all_to_all(sent, ("core", "heads"), 0, 0, tiled=True)
    read, picked = finish(device, back.reshape(shares, ny, *back.shape[1:]), knocked.T, nblk)
    return read.T, picked.T


def solution(mesh):
    inner = Mesh(mesh.devices.reshape(*KEY_AXES, mesh.devices.shape[1]), ("x", "z", "core", "heads"))
    keys = ("x", "z", "core")
    in_specs = (
        P(None, "heads", None),
        P(keys, "heads", None),
        P(keys, "heads", None),
        P("heads", keys),
        P(keys),
        P(),
    )
    out_specs = (P(None, keys), P())
    return jax.shard_map(body, mesh=inner, in_specs=in_specs, out_specs=out_specs, check_vma=False)
```

```python
import functools

import jax
import jax.numpy as jnp
from jax import lax
from jax.experimental import pallas as pl
from jax.experimental.pallas import tpu as pltpu
from jax.sharding import Mesh, PartitionSpec as P

BLOCK = 4096
KEY_AXES = (4, 4, 2)
NEG = -1e30
SCALE2 = 128 ** -0.5 * 1.4426950408889634
HIGH = lax.Precision.HIGHEST
F32 = jnp.float32


def iota(shape, dim):
    return lax.broadcasted_iota(jnp.int32, shape, dim)


def small(mib):
    return pltpu.CompilerParams(vmem_limit_bytes=int(mib * 2**20))


def attn_kernel(base_ref, qt, k_hbm, v_hbm, ms_ref, o_ref, sc, k_ref, v_ref, k_sem, v_sem, *, C, nblk, context, nq):
    total = k_ref.shape[0]
    rows = total // nblk
    R = qt.shape[1]
    hd = k_ref.shape[1]
    per = rows // C
    late = 2 * nq

    def copy(hbm, ref, sem, i):
        at = pl.ds(pl.multiple_of(i * C, C), C)
        return pltpu.make_async_copy(hbm.at[at, :], ref.at[at, :], sem.at[i])

    for b in range(nblk):
        for i in range(per):
            copy(k_hbm, k_ref, k_sem, b * per + i).start()
        for i in range(per):
            copy(v_hbm, v_ref, v_sem, b * per + i).start()

    even = (1 - (lax.broadcasted_iota(jnp.int32, (16, hd), 0) & 1)).astype(jnp.bfloat16)
    odd = 1 - even
    lane_even = (1 - (lax.broadcasted_iota(jnp.int32, (16, 128), 1) & 1)).astype(jnp.bfloat16)
    le = jnp.concatenate([lane_even] * (rows // 128), axis=1)[None]

    def masked(x):
        x3 = x.reshape(x.shape[0] // 16, 16, hd)
        return jnp.concatenate([(x3 * even[None]).reshape(x.shape), (x3 * odd[None]).reshape(x.shape)], axis=1)

    def top_of(s):
        return jnp.max(s.reshape(s.shape[0] // 8, 8, R), axis=0)

    def block(b, carry):
        here = pl.ds(pl.multiple_of(b * rows, rows), rows)
        for c in range(per):
            copy(k_hbm, k_ref, k_sem, b * per + c).wait()
        s = jnp.dot(masked(k_ref[here, :]), qt[...], preferred_element_type=jnp.float32) * SCALE2
        sc[...] = s
        early = top_of(s[:rows - late])

        def seen(_):
            tail = sc[rows - late:, :]
            key = lax.shift_right_logical(iota(tail.shape, 0), 1)
            query = lax.div(iota(tail.shape, 1), jnp.int32(R // nq))
            tail = jnp.where(key <= query, tail, NEG)
            sc[rows - late:, :] = tail
            return top_of(tail)

        last = base_ref[0] + (b + 1) * (rows // 2) == context
        mx = jnp.maximum(early, lax.cond(last, seen, lambda _: top_of(sc[rows - late:, :]), 0))
        mx = jnp.maximum(mx, pltpu.roll(mx, 2, 0))
        mx = jnp.maximum(mx, pltpu.roll(mx, 4, 0))

        for c in range(per):
            copy(v_hbm, v_ref, v_sem, b * per + c).wait()
        p = jnp.exp2(sc[...].reshape(rows // 8, 8, R) - mx[None])
        tot = jnp.sum(p, axis=0)
        pb = p.reshape(rows, R).astype(jnp.bfloat16)
        vt3 = v_ref[here, :].T.reshape(hd // 16, 16, rows)
        vt = jnp.concatenate([(vt3 * le).reshape(hd, rows), (vt3 * (1 - le)).reshape(hd, rows)], axis=0)
        o_ref[b] = jnp.dot(vt, pb, preferred_element_type=jnp.float32)
        tot = tot + pltpu.roll(tot, 2, 0)
        tot = tot + pltpu.roll(tot, 4, 0)
        ms_ref[b, 0:2, :] = mx[0:2]
        ms_ref[b, 2:4, :] = tot[0:2]
        return carry

    lax.fori_loop(0, nblk, block, 0)


def attention(base, qt, keys, values, block, context, nq, vl=48):
    n, kvh, hd = keys.shape
    R = qt.shape[1]
    C = kvh * block
    nblk = n // block
    rows = kvh * block
    k2 = keys.reshape(n * kvh, hd)
    v2 = values.reshape(n * kvh, hd)
    vmem = pl.BlockSpec(memory_space=pltpu.VMEM)
    hbm = pl.BlockSpec(memory_space=pltpu.HBM)
    return pl.pallas_call(
        functools.partial(attn_kernel, C=C, nblk=nblk, context=context, nq=nq),
        in_specs=[pl.BlockSpec(memory_space=pltpu.SMEM), vmem, hbm, hbm],
        out_specs=[vmem, vmem],
        out_shape=[
            jax.ShapeDtypeStruct((nblk, 4, R), jnp.float32),
            jax.ShapeDtypeStruct((nblk, kvh * hd, R), jnp.float32),
        ],
        scratch_shapes=[
            pltpu.VMEM((rows, R), jnp.float32),
            pltpu.VMEM((n * kvh, hd), jnp.bfloat16),
            pltpu.VMEM((n * kvh, hd), jnp.bfloat16),
            pltpu.SemaphoreType.DMA((n * kvh // C,)),
            pltpu.SemaphoreType.DMA((n * kvh // C,)),
        ],
        compiler_params=small(vl),
        cost_estimate=pl.CostEstimate(flops=4 * R * n * kvh * hd * 2, bytes_accessed=2 * n * kvh * hd * 2, transcendentals=R * n * kvh),
        name="attention",
    )(base, qt, k2, v2)


def direction_kernel(w_hbm, p_hbm, q_hbm, out_hbm, qt_ref, w, p, q, out, sem):
    count = sem.shape[0] - 3
    step = w.shape[0] // count
    first = pltpu.make_async_copy(p_hbm, p, sem.at[count])
    queries = pltpu.make_async_copy(q_hbm, q, sem.at[count + 1])
    first.start()
    copies = []
    for i in range(count):
        at = pl.ds(i * step, step)
        copies.append(pltpu.make_async_copy(w_hbm.at[at, :], w.at[at, :], sem.at[i]))
        copies[-1].start()
    queries.start()
    hd = out.shape[2]
    first.wait()
    probe = jnp.broadcast_to(p[...].astype(F32).reshape(1, w.shape[1]), (8, w.shape[1])).astype(jnp.bfloat16)
    rows = []
    for i, c in enumerate(copies):
        c.wait()
        part = lax.dot_general(probe, w[i * step:(i + 1) * step, :], (((1,), (1,)), ((), ())), preferred_element_type=F32)
        rows += [part[0:1, h * hd:(h + 1) * hd] for h in range(step // hd)]
    full = jnp.concatenate(rows, axis=0)
    for dest in range(out.shape[0]):
        out[dest] = full
    back = pltpu.make_async_copy(out, out_hbm, sem.at[count + 2])
    back.start()
    queries.wait()
    x = q[...].astype(F32)
    g = x.shape[1] // 2
    R = x.shape[0] * g
    both = jnp.concatenate([x[:, :g].reshape(R, hd), x[:, g:].reshape(R, hd)], axis=1)
    qt_ref[...] = both.T.astype(jnp.bfloat16)
    back.wait()


def direction_parts(out_weight, probe, queries, dests):
    rows, cols = out_weight.shape
    nq, hq, hd = queries.shape
    vmem = pl.BlockSpec(memory_space=pltpu.VMEM)
    hbm = pl.BlockSpec(memory_space=pltpu.HBM)
    return pl.pallas_call(
        direction_kernel,
        in_specs=[hbm, hbm, hbm],
        out_specs=[hbm, vmem],
        out_shape=[
            jax.ShapeDtypeStruct((dests, rows // hd, hd), F32),
            jax.ShapeDtypeStruct((2 * hd, nq * hq // 2), jnp.bfloat16),
        ],
        scratch_shapes=[
            pltpu.VMEM(out_weight.shape, jnp.bfloat16),
            pltpu.VMEM(probe.shape, jnp.bfloat16),
            pltpu.VMEM(queries.shape, jnp.bfloat16),
            pltpu.VMEM((dests, rows // hd, hd), F32),
            pltpu.SemaphoreType.DMA((7,)),
        ],
        cost_estimate=pl.CostEstimate(flops=2 * rows * cols, bytes_accessed=rows * cols * 2, transcendentals=0),
        compiler_params=small(53.25),
        name="direction",
    )(out_weight, probe, queries)


def pack_kernel(dir_ref, ms_ref, o_ref, out_ref, x):
    nblk, rows, R = o_ref.shape
    heads, hd = dir_ref.shape[1:]
    group = heads // 2
    direction = jnp.sum(dir_ref[...], axis=0)
    spread = (iota((group, 128), 1) & (group - 1)) == iota((group, 128), 0)
    spread = spread.astype(F32)
    for g in range(2):
        wide = lax.dot_general(direction[g * group:(g + 1) * group], spread, (((0,), (0,)), ((), ())),
                               preferred_element_type=F32, precision=HIGH)
        for b in range(nblk):
            at = g * nblk + b
            x[at:at + 1, :] = ms_ref[b, g:g + 1, :]
            x[8 + at:9 + at, :] = ms_ref[b, 2 + g:3 + g, :]
            for c in range(0, R, 128):
                part = o_ref[b, g * hd:(g + 1) * hd, c:c + 128] * wide
                x[16 + at:17 + at, c:c + 128] = jnp.sum(part, axis=0, keepdims=True)
    total = x[8:16, :]
    level = x[0:8, :] + jnp.log2(total)
    mean = x[16:24, :] / total
    dests = out_ref.shape[0]
    wide = out_ref.shape[2]
    for dest in range(dests):
        c = dest % (R // wide) * wide
        out_ref[dest, 0:8, :] = level[:, c:c + wide]
        out_ref[dest, 8:16, :] = mean[:, c:c + wide]


def pack(gathered, ms, o, shares):
    dests = gathered.shape[0]
    R = ms.shape[2]
    return pl.pallas_call(
        pack_kernel,
        out_shape=jax.ShapeDtypeStruct((dests, 16, R // shares), F32),
        scratch_shapes=[pltpu.VMEM((24, R), F32)],
        cost_estimate=pl.CostEstimate(flops=2 * o.size, bytes_accessed=o.size * 4, transcendentals=0),
        compiler_params=small(8),
        name="pack",
    )(gathered, ms, o)


def turned(x, k):
    row = iota(x.shape, x.ndim - 2) & 3
    return jnp.where(row >= k, pltpu.roll(x, k, x.ndim - 2), pltpu.roll(x, k + 4, x.ndim - 2))


def around(x, op):
    x = op(x, turned(x, 1))
    return op(x, turned(x, 2))


def out_of_sources(x):
    n = x.shape[0]
    before = [jnp.zeros_like(x[0])]
    after = [jnp.zeros_like(x[0])]
    for k in range(n - 1):
        before.append(before[-1] + x[k])
        after.insert(0, after[0] + x[n - 1 - k])
    return jnp.stack([p + q for p, q in zip(before, after)], axis=0)


def leave_kernel(got_ref, out_ref):
    level = got_ref[:, 0:8, :]
    mean = got_ref[:, 8:16, :]
    n, _, lanes = level.shape
    top = around(jnp.max(level, axis=0), jnp.maximum)
    is_top = level == top[None]
    count = around(jnp.sum(is_top.astype(F32), axis=0), jnp.add)
    second = around(jnp.max(jnp.where(is_top, NEG, level), axis=0), jnp.maximum)
    factor = jnp.exp2(level - top[None])
    low = jnp.where(is_top, 0.0, jnp.exp2(jnp.minimum(level - second[None], 0.0)))
    alone = is_top & (count == 1.0)[None]

    def left_out(a, rest):
        inner = turned(a, 1) + turned(a, 2) + turned(a, 3)
        shared = inner + out_of_sources(a + inner)
        rest = around(jnp.sum(rest, axis=0), jnp.add)
        return jnp.where(alone, rest[None], shared)

    ratio = left_out(mean * factor, mean * low) / left_out(factor, low)
    both = ratio + pltpu.roll(ratio, 4, 1)
    pairs = both.reshape(n // 2, 2, 8, lanes)
    dense = jnp.where(iota((n // 2, 8, lanes), 1) < 4, pairs[:, 0], pairs[:, 1]).reshape(n * 4, lanes)
    queries = out_ref.shape[1]
    per = lanes // queries
    pick = lax.div(iota((queries, lanes), 1), jnp.int32(per)) == iota((queries, lanes), 0)
    part = lax.dot_general(pick.astype(F32), dense, (((1,), (1,)), ((), ())), preferred_element_type=F32, precision=HIGH)
    for dest in range(out_ref.shape[0]):
        out_ref[dest] = part


def leave(got, queries, dests):
    return pl.pallas_call(
        leave_kernel,
        out_shape=jax.ShapeDtypeStruct((dests, queries, got.shape[0] * 4), F32),
        cost_estimate=pl.CostEstimate(flops=8 * got.size, bytes_accessed=got.size * 4, transcendentals=got.size),
        compiler_params=small(8),
        name="leave",
    )(got)


def finish_kernel(device_ref, got_ref, knocked_ref, read_ref, pick_ref):
    nx, ny, q, nb = got_ref.shape
    parts = []
    for i in range(nx):
        total = got_ref[i, 0]
        for j in range(1, ny):
            total = total + got_ref[i, j]
        parts.append(total)
    full = jnp.concatenate(parts, axis=0).T
    block = iota(full.shape, 0)
    for k in range(pick_ref.shape[0]):
        here = jnp.where(block == knocked_ref[k:k + 1, :], full, 0.0)
        pick_ref[k:k + 1, :] = jnp.sum(here, axis=0, keepdims=True)
    nblk = read_ref.shape[0]
    for t in range(nblk):
        here = jnp.where(block == device_ref[0] * nblk + t, full, 0.0)
        read_ref[t:t + 1, :] = jnp.sum(here, axis=0, keepdims=True)


def finish(device, got, knocked_t, nblk):
    nx, ny, q, nb = got.shape
    vmem = pl.BlockSpec(memory_space=pltpu.VMEM)
    return pl.pallas_call(
        finish_kernel,
        in_specs=[pl.BlockSpec(memory_space=pltpu.SMEM), vmem, vmem],
        out_specs=[vmem, vmem],
        out_shape=[jax.ShapeDtypeStruct((nblk, nx * q), F32), jax.ShapeDtypeStruct(knocked_t.shape, F32)],
        compiler_params=small(2),
        name="finish",
    )(device, got, knocked_t)


def body(queries, keys, values, out_weight, probe, knocked):
    nq, hq, hd = queries.shape
    nblk = keys.shape[0] // BLOCK
    axes = ("x", "z", "core")
    lanes = lax.axis_size(axes)
    device = lax.axis_index(axes).reshape(1)
    context = keys.shape[0] * lanes
    parts, qt = direction_parts(out_weight, probe, queries, lanes)
    gathered = lax.all_to_all(parts, axes, 0, 0, tiled=True)
    ms, o = attention(device * keys.shape[0], qt, keys, values, BLOCK, context, nq)
    shares, ny = lax.axis_size("core"), lax.axis_size("heads")
    got = lax.all_to_all(pack(gathered, ms, o, shares), axes, 0, 0, tiled=True)
    sent = leave(got, nq // shares, shares * ny)
    back = lax.all_to_all(sent, ("core", "heads"), 0, 0, tiled=True)
    read, picked = finish(device, back.reshape(shares, ny, *back.shape[1:]), knocked.T, nblk)
    return read.T, picked.T


def solution(mesh):
    inner = Mesh(mesh.devices.reshape(*KEY_AXES, mesh.devices.shape[1]), ("x", "z", "core", "heads"))
    keys = ("x", "z", "core")
    in_specs = (
        P(None, "heads", None),
        P(keys, "heads", None),
        P(keys, "heads", None),
        P("heads", keys),
        P(keys),
        P(),
    )
    out_specs = (P(None, keys), P())
    return jax.shard_map(body, mesh=inner, in_specs=in_specs, out_specs=out_specs, check_vma=False)
```

```python
import functools

import jax
import jax.numpy as jnp
from jax import lax
from jax.experimental import pallas as pl
from jax.experimental.pallas import tpu as pltpu
from jax.sharding import Mesh, PartitionSpec as P

BLOCK = 4096
KEY_AXES = (4, 4, 2)
NEG = -1e30
SCALE2 = 128 ** -0.5 * 1.4426950408889634
HIGH = lax.Precision.HIGHEST
F32 = jnp.float32


def iota(shape, dim):
    return lax.broadcasted_iota(jnp.int32, shape, dim)


def small(mib):
    return pltpu.CompilerParams(vmem_limit_bytes=int(mib * 2**20))


def attn_kernel(base_ref, qt, k_hbm, v_hbm, ms_ref, o_ref, sc, k_ref, v_ref, k_sem, v_sem, *, C, nblk, context, nq):
    total = k_ref.shape[0]
    rows = total // nblk
    R = qt.shape[1]
    hd = k_ref.shape[1]
    per = rows // C
    late = 2 * nq

    def copy(hbm, ref, sem, i):
        at = pl.ds(pl.multiple_of(i * C, C), C)
        return pltpu.make_async_copy(hbm.at[at, :], ref.at[at, :], sem.at[i])

    for b in range(nblk):
        for i in range(per):
            copy(k_hbm, k_ref, k_sem, b * per + i).start()
        for i in range(per):
            copy(v_hbm, v_ref, v_sem, b * per + i).start()

    even = (1 - (lax.broadcasted_iota(jnp.int32, (16, hd), 0) & 1)).astype(jnp.bfloat16)
    odd = 1 - even
    lane_even = (1 - (lax.broadcasted_iota(jnp.int32, (16, 128), 1) & 1)).astype(jnp.bfloat16)
    le = jnp.concatenate([lane_even] * (rows // 128), axis=1)[None]

    def masked(x):
        x3 = x.reshape(x.shape[0] // 16, 16, hd)
        return jnp.concatenate([(x3 * even[None]).reshape(x.shape), (x3 * odd[None]).reshape(x.shape)], axis=1)

    def top_of(s):
        return jnp.max(s.reshape(s.shape[0] // 8, 8, R), axis=0)

    def block(b, carry):
        here = pl.ds(pl.multiple_of(b * rows, rows), rows)
        for c in range(per):
            copy(k_hbm, k_ref, k_sem, b * per + c).wait()
        s = jnp.dot(masked(k_ref[here, :]), qt[...], preferred_element_type=jnp.float32) * SCALE2
        sc[...] = s
        early = top_of(s[:rows - late])

        def seen(_):
            tail = sc[rows - late:, :]
            key = lax.shift_right_logical(iota(tail.shape, 0), 1)
            query = lax.div(iota(tail.shape, 1), jnp.int32(R // nq))
            tail = jnp.where(key <= query, tail, NEG)
            sc[rows - late:, :] = tail
            return top_of(tail)

        last = base_ref[0] + (b + 1) * (rows // 2) == context
        mx = jnp.maximum(early, lax.cond(last, seen, lambda _: top_of(sc[rows - late:, :]), 0))
        mx = jnp.maximum(mx, pltpu.roll(mx, 2, 0))
        mx = jnp.maximum(mx, pltpu.roll(mx, 4, 0))

        for c in range(per):
            copy(v_hbm, v_ref, v_sem, b * per + c).wait()
        p = jnp.exp2(sc[...].reshape(rows // 8, 8, R) - mx[None])
        tot = jnp.sum(p, axis=0)
        pb = p.reshape(rows, R).astype(jnp.bfloat16)
        vt3 = v_ref[here, :].T.reshape(hd // 16, 16, rows)
        vt = jnp.concatenate([(vt3 * le).reshape(hd, rows), (vt3 * (1 - le)).reshape(hd, rows)], axis=0)
        o_ref[b] = jnp.dot(vt, pb, preferred_element_type=jnp.float32)
        tot = tot + pltpu.roll(tot, 2, 0)
        tot = tot + pltpu.roll(tot, 4, 0)
        ms_ref[b, 0:2, :] = mx[0:2]
        ms_ref[b, 2:4, :] = tot[0:2]
        return carry

    lax.fori_loop(0, nblk, block, 0)


def attention(base, qt, keys, values, block, context, nq, vl=48):
    n, kvh, hd = keys.shape
    R = qt.shape[1]
    C = kvh * block
    nblk = n // block
    rows = kvh * block
    k2 = keys.reshape(n * kvh, hd)
    v2 = values.reshape(n * kvh, hd)
    vmem = pl.BlockSpec(memory_space=pltpu.VMEM)
    hbm = pl.BlockSpec(memory_space=pltpu.HBM)
    return pl.pallas_call(
        functools.partial(attn_kernel, C=C, nblk=nblk, context=context, nq=nq),
        in_specs=[pl.BlockSpec(memory_space=pltpu.SMEM), vmem, hbm, hbm],
        out_specs=[vmem, vmem],
        out_shape=[
            jax.ShapeDtypeStruct((nblk, 4, R), jnp.float32),
            jax.ShapeDtypeStruct((nblk, kvh * hd, R), jnp.float32),
        ],
        scratch_shapes=[
            pltpu.VMEM((rows, R), jnp.float32),
            pltpu.VMEM((n * kvh, hd), jnp.bfloat16),
            pltpu.VMEM((n * kvh, hd), jnp.bfloat16),
            pltpu.SemaphoreType.DMA((n * kvh // C,)),
            pltpu.SemaphoreType.DMA((n * kvh // C,)),
        ],
        compiler_params=small(vl),
        cost_estimate=pl.CostEstimate(flops=4 * R * n * kvh * hd * 2, bytes_accessed=2 * n * kvh * hd * 2, transcendentals=R * n * kvh),
        name="attention",
    )(base, qt, k2, v2)


def direction_kernel(w_hbm, p_hbm, q_hbm, out_hbm, qt_ref, w, p, q, out, sem):
    count = sem.shape[0] - 3
    step = w.shape[0] // count
    first = pltpu.make_async_copy(p_hbm, p, sem.at[count])
    queries = pltpu.make_async_copy(q_hbm, q, sem.at[count + 1])
    first.start()
    copies = []
    for i in range(count):
        at = pl.ds(i * step, step)
        copies.append(pltpu.make_async_copy(w_hbm.at[at, :], w.at[at, :], sem.at[i]))
        copies[-1].start()
    queries.start()
    hd = out.shape[2]
    first.wait()
    probe = jnp.broadcast_to(p[...].astype(F32).reshape(1, w.shape[1]), (8, w.shape[1])).astype(jnp.bfloat16)
    rows = []
    for i, c in enumerate(copies):
        c.wait()
        part = lax.dot_general(probe, w[i * step:(i + 1) * step, :], (((1,), (1,)), ((), ())), preferred_element_type=F32)
        rows += [part[0:1, h * hd:(h + 1) * hd] for h in range(step // hd)]
    full = jnp.concatenate(rows, axis=0)
    for dest in range(out.shape[0]):
        out[dest] = full
    back = pltpu.make_async_copy(out, out_hbm, sem.at[count + 2])
    back.start()
    queries.wait()
    x = q[...].astype(F32)
    g = x.shape[1] // 2
    R = x.shape[0] * g
    both = jnp.concatenate([x[:, :g].reshape(R, hd), x[:, g:].reshape(R, hd)], axis=1)
    qt_ref[...] = both.T.astype(jnp.bfloat16)
    back.wait()


def direction_parts(out_weight, probe, queries, dests):
    rows, cols = out_weight.shape
    nq, hq, hd = queries.shape
    vmem = pl.BlockSpec(memory_space=pltpu.VMEM)
    hbm = pl.BlockSpec(memory_space=pltpu.HBM)
    return pl.pallas_call(
        direction_kernel,
        in_specs=[hbm, hbm, hbm],
        out_specs=[hbm, vmem],
        out_shape=[
            jax.ShapeDtypeStruct((dests, rows // hd, hd), F32),
            jax.ShapeDtypeStruct((2 * hd, nq * hq // 2), jnp.bfloat16),
        ],
        scratch_shapes=[
            pltpu.VMEM(out_weight.shape, jnp.bfloat16),
            pltpu.VMEM(probe.shape, jnp.bfloat16),
            pltpu.VMEM(queries.shape, jnp.bfloat16),
            pltpu.VMEM((dests, rows // hd, hd), F32),
            pltpu.SemaphoreType.DMA((5,)),
        ],
        cost_estimate=pl.CostEstimate(flops=2 * rows * cols, bytes_accessed=rows * cols * 2, transcendentals=0),
        compiler_params=small(53.25),
        name="direction",
    )(out_weight, probe, queries)


def pack_kernel(dir_ref, ms_ref, o_ref, out_ref, x):
    nblk, rows, R = o_ref.shape
    heads, hd = dir_ref.shape[1:]
    group = heads // 2
    direction = jnp.sum(dir_ref[...], axis=0)
    spread = (iota((group, 128), 1) & (group - 1)) == iota((group, 128), 0)
    spread = spread.astype(F32)
    for g in range(2):
        wide = lax.dot_general(direction[g * group:(g + 1) * group], spread, (((0,), (0,)), ((), ())),
                               preferred_element_type=F32, precision=HIGH)
        for b in range(nblk):
            at = g * nblk + b
            x[at:at + 1, :] = ms_ref[b, g:g + 1, :]
            x[8 + at:9 + at, :] = ms_ref[b, 2 + g:3 + g, :]
            for c in range(0, R, 128):
                part = o_ref[b, g * hd:(g + 1) * hd, c:c + 128] * wide
                x[16 + at:17 + at, c:c + 128] = jnp.sum(part, axis=0, keepdims=True)
    total = x[8:16, :]
    level = x[0:8, :] + jnp.log2(total)
    mean = x[16:24, :] / total
    dests = out_ref.shape[0]
    wide = out_ref.shape[2]
    for dest in range(dests):
        c = dest % (R // wide) * wide
        out_ref[dest, 0:8, :] = level[:, c:c + wide]
        out_ref[dest, 8:16, :] = mean[:, c:c + wide]


def pack(gathered, ms, o, shares):
    dests = gathered.shape[0]
    R = ms.shape[2]
    return pl.pallas_call(
        pack_kernel,
        out_shape=jax.ShapeDtypeStruct((dests, 16, R // shares), F32),
        scratch_shapes=[pltpu.VMEM((24, R), F32)],
        cost_estimate=pl.CostEstimate(flops=2 * o.size, bytes_accessed=o.size * 4, transcendentals=0),
        compiler_params=small(8),
        name="pack",
    )(gathered, ms, o)


def turned(x, k):
    row = iota(x.shape, x.ndim - 2) & 3
    return jnp.where(row >= k, pltpu.roll(x, k, x.ndim - 2), pltpu.roll(x, k + 4, x.ndim - 2))


def around(x, op):
    x = op(x, turned(x, 1))
    return op(x, turned(x, 2))


def out_of_sources(x):
    n = x.shape[0]
    before = [jnp.zeros_like(x[0])]
    after = [jnp.zeros_like(x[0])]
    for k in range(n - 1):
        before.append(before[-1] + x[k])
        after.insert(0, after[0] + x[n - 1 - k])
    return jnp.stack([p + q for p, q in zip(before, after)], axis=0)


def leave_kernel(got_ref, out_ref):
    level = got_ref[:, 0:8, :]
    mean = got_ref[:, 8:16, :]
    n, _, lanes = level.shape
    top = around(jnp.max(level, axis=0), jnp.maximum)
    is_top = level == top[None]
    count = around(jnp.sum(is_top.astype(F32), axis=0), jnp.add)
    second = around(jnp.max(jnp.where(is_top, NEG, level), axis=0), jnp.maximum)
    factor = jnp.exp2(level - top[None])
    low = jnp.where(is_top, 0.0, jnp.exp2(jnp.minimum(level - second[None], 0.0)))
    alone = is_top & (count == 1.0)[None]

    def left_out(a, rest):
        inner = turned(a, 1) + turned(a, 2) + turned(a, 3)
        shared = inner + out_of_sources(a + inner)
        rest = around(jnp.sum(rest, axis=0), jnp.add)
        return jnp.where(alone, rest[None], shared)

    ratio = left_out(mean * factor, mean * low) / left_out(factor, low)
    both = ratio + pltpu.roll(ratio, 4, 1)
    pairs = both.reshape(n // 2, 2, 8, lanes)
    dense = jnp.where(iota((n // 2, 8, lanes), 1) < 4, pairs[:, 0], pairs[:, 1]).reshape(n * 4, lanes)
    queries = out_ref.shape[1]
    per = lanes // queries
    pick = lax.div(iota((queries, lanes), 1), jnp.int32(per)) == iota((queries, lanes), 0)
    part = lax.dot_general(pick.astype(F32), dense, (((1,), (1,)), ((), ())), preferred_element_type=F32, precision=HIGH)
    for dest in range(out_ref.shape[0]):
        out_ref[dest] = part


def leave(got, queries, dests):
    return pl.pallas_call(
        leave_kernel,
        out_shape=jax.ShapeDtypeStruct((dests, queries, got.shape[0] * 4), F32),
        cost_estimate=pl.CostEstimate(flops=8 * got.size, bytes_accessed=got.size * 4, transcendentals=got.size),
        compiler_params=small(8),
        name="leave",
    )(got)


def finish_kernel(device_ref, got_ref, knocked_ref, read_ref, pick_ref):
    nx, ny, q, nb = got_ref.shape
    parts = []
    for i in range(nx):
        total = got_ref[i, 0]
        for j in range(1, ny):
            total = total + got_ref[i, j]
        parts.append(total)
    full = jnp.concatenate(parts, axis=0).T
    block = iota(full.shape, 0)
    for k in range(pick_ref.shape[0]):
        here = jnp.where(block == knocked_ref[k:k + 1, :], full, 0.0)
        pick_ref[k:k + 1, :] = jnp.sum(here, axis=0, keepdims=True)
    nblk = read_ref.shape[0]
    for t in range(nblk):
        here = jnp.where(block == device_ref[0] * nblk + t, full, 0.0)
        read_ref[t:t + 1, :] = jnp.sum(here, axis=0, keepdims=True)


def finish(device, got, knocked_t, nblk):
    nx, ny, q, nb = got.shape
    vmem = pl.BlockSpec(memory_space=pltpu.VMEM)
    return pl.pallas_call(
        finish_kernel,
        in_specs=[pl.BlockSpec(memory_space=pltpu.SMEM), vmem, vmem],
        out_specs=[vmem, vmem],
        out_shape=[jax.ShapeDtypeStruct((nblk, nx * q), F32), jax.ShapeDtypeStruct(knocked_t.shape, F32)],
        compiler_params=small(2),
        name="finish",
    )(device, got, knocked_t)


def body(queries, keys, values, out_weight, probe, knocked):
    nq, hq, hd = queries.shape
    nblk = keys.shape[0] // BLOCK
    axes = ("x", "z", "core")
    lanes = lax.axis_size(axes)
    device = lax.axis_index(axes).reshape(1)
    context = keys.shape[0] * lanes
    parts, qt = direction_parts(out_weight, probe, queries, lanes)
    gathered = lax.all_to_all(parts, axes, 0, 0, tiled=True)
    ms, o = attention(device * keys.shape[0], qt, keys, values, BLOCK, context, nq)
    shares, ny = lax.axis_size("core"), lax.axis_size("heads")
    got = lax.all_to_all(pack(gathered, ms, o, shares), axes, 0, 0, tiled=True)
    sent = leave(got, nq // shares, shares * ny)
    back = lax.all_to_all(sent, ("core", "heads"), 0, 0, tiled=True)
    read, picked = finish(device, back.reshape(shares, ny, *back.shape[1:]), knocked.T, nblk)
    return read.T, picked.T


def solution(mesh):
    inner = Mesh(mesh.devices.reshape(*KEY_AXES, mesh.devices.shape[1]), ("x", "z", "core", "heads"))
    keys = ("x", "z", "core")
    in_specs = (
        P(None, "heads", None),
        P(keys, "heads", None),
        P(keys, "heads", None),
        P("heads", keys),
        P(keys),
        P(),
    )
    out_specs = (P(None, keys), P())
    return jax.shard_map(body, mesh=inner, in_specs=in_specs, out_specs=out_specs, check_vma=False)
```
